512 devices in a mesh: prow: 16 (over z, core), pcol: 32 (over y, x).
Axes of the slice: x: 4, y: 8, z: 8, core: 2. Of those that a mesh axis runs over, the one named last changes fastest.
Arguments:
- tiles: bfloat16 [16, 32, 32, 256, 256], P('prow', 'pcol')
- tile_brow: int32 [16, 32, 32], P('prow', 'pcol'), may hold values from 0 to 31, as said below
- tile_bcol: int32 [16, 32, 32], P('prow', 'pcol'), may hold values from 0 to 15, as said below
- tile_count: int32 [16, 32], P('prow', 'pcol'), may hold values from 8 to 32, as said below
Outputs:
- row_scale: float32 [32, 16, 256], P(None, 'prow')
- col_scale: float32 [16, 32, 256], P(None, 'pcol')
The draws below stay inside these ranges and needn't reach their ends.
Inputs may be any that keep to these rules, and one draw needn't show every extreme that they name: `tile_brow`: on one device, no two slots name the same pair of local block row and column; the diagonal tile of every block row is present and live, in the first slots of the device that holds it. `tile_bcol`: see tile_brow. `tile_count`: a device that holds diagonal tiles has all 32 slots live, every other device at most 16.
All inputs are finite; a program needn't handle non-finite values.
Results may differ from the reference program's by a relative error of at most 0.0003.
Values sent between devices are 32-bit elements; how exact they have to be, the bound alone decides.
A program may use at most 64 MiB of HBM per device.

```python
import jax
import jax.numpy as jnp
from jax import lax

TILE = 256
BR_DEV = 32
TILES_DEV = 32
SWEEPS = 3
BC_DEV = 16
N_PROW = 16
N_PCOL = 32


def draw_tiles(key, part):
    shape = (N_PROW, N_PCOL, TILES_DEV, TILE, TILE)
    base = jax.random.normal(jax.random.fold_in(key, 11), shape, jnp.float32)
    span = 2.3
    row_log = jax.random.uniform(jax.random.fold_in(key, 12), (N_PROW, N_PCOL, TILES_DEV, TILE, 1), jnp.float32, -span, span)
    col_log = jax.random.uniform(jax.random.fold_in(key, 13), (N_PROW, N_PCOL, TILES_DEV, 1, TILE), jnp.float32, -span, span)
    return (base * jnp.exp(row_log) * jnp.exp(col_log)).astype(jnp.bfloat16)


def place_slots(key):
    cells = BR_DEV * BC_DEV
    keys = jax.random.split(jax.random.fold_in(key, 21), N_PROW * N_PCOL)
    cell_ids = jnp.arange(cells, dtype=jnp.int32)
    rows_of = cell_ids // BC_DEV
    cols_of = cell_ids % BC_DEV

    def one_device(device_key, position):
        prow_id = position // N_PCOL
        pcol_id = position % N_PCOL
        diagonal = rows_of * N_PROW + prow_id == cols_of * N_PCOL + pcol_id
        order = jax.random.permutation(device_key, cells).astype(jnp.int32)
        score = jnp.where(diagonal, order - cells, order)
        chosen = jnp.argsort(score, stable=True)[:TILES_DEV].astype(jnp.int32)
        return (rows_of[chosen], cols_of[chosen])
    brows, bcols = jax.vmap(one_device)(keys, jnp.arange(N_PROW * N_PCOL, dtype=jnp.int32))
    return (brows.reshape(N_PROW, N_PCOL, TILES_DEV), bcols.reshape(N_PROW, N_PCOL, TILES_DEV))


def draw_tile_brow(key, part):
    return place_slots(key)[0].astype(jnp.int32)


def draw_tile_bcol(key, part):
    return place_slots(key)[1].astype(jnp.int32)


def draw_tile_count(key, part):
    low = max(TILES_DEV // 4, 1)
    high = max(TILES_DEV // 2, low)
    counts = jax.random.randint(jax.random.fold_in(key, 31), (N_PROW, N_PCOL), low, high + 1)
    prow_ids = jnp.arange(N_PROW, dtype=jnp.int32)[:, None]
    pcol_ids = jnp.arange(N_PCOL, dtype=jnp.int32)[None, :]
    holder = pcol_ids % N_PROW == prow_ids
    return jnp.where(holder, TILES_DEV, counts).astype(jnp.int32)


def setup_inputs(seed: int = 0) -> dict:
    key_list = jax.random.split(jax.random.key(seed), 5)
    return {
        "tiles": draw_tiles(jax.random.fold_in(key_list[4], 71), 0),
        "tile_brow": draw_tile_brow(jax.random.fold_in(key_list[4], 71), 0),
        "tile_bcol": draw_tile_bcol(jax.random.fold_in(key_list[4], 71), 0),
        "tile_count": draw_tile_count(jax.random.fold_in(key_list[4], 71), 0),
    }


def rescale(scale, largest):
    return scale / jnp.sqrt(largest)

def reference(tiles, tile_brow, tile_bcol, tile_count):
    live = (jnp.arange(TILES_DEV, dtype=jnp.int32)[None, None, :] < tile_count[:, :, None]).astype(jnp.float32)
    row_vec = jnp.ones((N_PROW, BR_DEV, TILE), jnp.float32)
    col_vec = jnp.ones((N_PCOL, BC_DEV, TILE), jnp.float32)
    col_ids = jnp.arange(N_PCOL, dtype=jnp.int32)[:, None]
    for sweep in range(SWEEPS):

        def one_row(inputs):
            block, brow, bcol, alive, rows = inputs
            row_take = rows[brow]
            col_take = col_vec[col_ids, bcol]
            scaled = jnp.abs(block.astype(jnp.float32)) * row_take[:, :, :, None] * col_take[:, :, None, :]
            row_part = lax.optimization_barrier(jnp.max(scaled, axis=3)) * alive[:, :, None]
            col_part = lax.optimization_barrier(jnp.max(scaled, axis=2)) * alive[:, :, None]
            row_new = jnp.zeros((BR_DEV, TILE), jnp.float32).at[brow.reshape(-1)].max(row_part.reshape(-1, TILE))
            col_new = jnp.zeros((N_PCOL, BC_DEV, TILE), jnp.float32).at[jnp.broadcast_to(col_ids, bcol.shape).reshape(-1), bcol.reshape(-1)].max(col_part.reshape(-1, TILE))
            return (row_new, col_new)
        row_max, col_parts = lax.map(one_row, (tiles, tile_brow, tile_bcol, live, row_vec))
        col_max = lax.optimization_barrier(jnp.max(col_parts, axis=0))
        row_vec = rescale(row_vec, row_max)
        col_vec = rescale(col_vec, col_max)
    return (jnp.transpose(row_vec, (1, 0, 2)), jnp.transpose(col_vec, (1, 0, 2)))
```

```python
import functools

import jax
import jax.numpy as jnp
from jax import lax
from jax.experimental import pallas as pl
from jax.experimental.pallas import tpu as pltpu
from jax.sharding import PartitionSpec as P

MESH = pl.DeviceIdType.MESH
SWEEPS = 3
NX, NY, NZ, NC = 4, 8, 8, 2
PIECES, BLOCKS = 4, 8
LIFT = 2.0**63
KNEE = 2.0**64


def kernel(
    count_ref, brow_ref, bcol_ref, tiles_hbm, row_ref, col_ref,
    tiles, turned, row_u, row_v, col_u, col_v,
    rs_src, rs_got, plane, along, pair_src, pair_got,
    load_sem, send_sem, rs_sem, plane_sem, along_sem, pair_sem,
):
    slots, width = tiles.shape[0], tiles.shape[1]
    half = width // 2
    brs, bcs = row_ref.shape[0], col_ref.shape[0]
    piece = brs // PIECES
    prow, pcol = lax.axis_index("prow"), lax.axis_index("pcol")
    z, core = prow // NC, prow % NC
    y, x = pcol // NX, pcol % NX
    part = (y % 2) * 2 + x % 2
    block = (y // 2) * 2 + x // 2
    mine = part * BLOCKS + block

    loads = [
        pltpu.make_async_copy(tiles_hbm.at[s], tiles.at[s], load_sem.at[s])
        for s in range(slots)
    ]
    for load in loads:
        load.start()

    near = []
    for d in range(1, 4):
        px = x + (1 - 2 * (x % 2)) * (d % 2)
        py = y + (1 - 2 * (y % 2)) * (d // 2)
        near.append(((py % 2) * 2 + px % 2, (prow, py * NX + px)))
    offsets = [(dy, dx) for dy in range(NY) for dx in range(NX) if (dy, dx) != (0, 0)]
    offsets.sort(key=lambda o: -(min(o[0], NY - o[0]) + min(o[1], NX - o[1])))
    flat = [
        (prow, lax.rem(y + dy, NY) * NX + lax.rem(x + dx, NX)) for dy, dx in offsets
    ]
    steps = sorted(range(1, NZ), key=lambda d: -min(d, NZ - d))
    up = [(lax.rem(z + d, NZ) * NC + core, pcol) for d in steps]
    partner = (z * NC + 1 - core, pcol)

    barrier = pltpu.get_barrier_semaphore()
    everyone = flat + up + [partner]
    for device in everyone:
        pl.semaphore_signal(barrier, inc=1, device_id=device, device_id_type=MESH)

    count = count_ref[0]
    row_iota = lax.broadcasted_iota(jnp.int32, (brs, width), 0)
    col_iota = lax.broadcasted_iota(jnp.int32, (bcs, width), 0)

    def put(total, iota, where_to, s, value):
        place = jnp.where(s < count, where_to, -1)
        return jnp.maximum(total, jnp.where(iota == place, value, 0.0))

    def first(s, totals):
        rows, cols = totals
        tile = jnp.abs(tiles[s])
        tiles[s] = tile
        flip = tile.T
        turned[s] = flip
        rows = put(rows, row_iota, brow_ref[s], s, jnp.max(flip, axis=0, keepdims=True).astype(jnp.float32))
        cols = put(cols, col_iota, bcol_ref[s], s, jnp.max(tile, axis=0, keepdims=True).astype(jnp.float32))
        return rows, cols

    totals = (jnp.zeros((brs, width), jnp.float32), jnp.zeros((bcs, width), jnp.float32))
    for s in range(slots):
        loads[s].wait()
        totals = first(s, totals)
    rows, cols = totals

    def copy(src, dst, sem, device):
        pltpu.make_async_remote_copy(
            src_ref=src, dst_ref=dst, send_sem=send_sem, recv_sem=sem,
            device_id=device, device_id_type=MESH,
        ).start()

    def took(ref, sem):
        pltpu.make_async_copy(ref, ref, sem).wait()

    def row_scatter(sweep, value):
        rs_src[sweep] = value
        for d, (k, device) in enumerate(near):
            copy(rs_src.at[sweep, pl.ds(pl.multiple_of(k * piece, piece), piece)],
                 rs_got.at[sweep, d], rs_sem.at[sweep], device)

    def row_spread(sweep):
        took(rs_got.at[sweep], rs_sem.at[sweep])
        value = rs_src[sweep, pl.ds(pl.multiple_of(part * piece, piece), piece)]
        for d in range(3):
            value = jnp.maximum(value, rs_got[sweep, d])
        plane[sweep, mine] = value
        for device in flat:
            copy(plane.at[sweep, mine], plane.at[sweep, mine], plane_sem.at[sweep], device)

    def row_result(sweep):
        took(plane.at[sweep, pl.ds(0, len(flat))], plane_sem.at[sweep])
        pieces = []
        for k in range(PIECES):
            value = plane[sweep, k * BLOCKS]
            for b in range(1, BLOCKS):
                value = jnp.maximum(value, plane[sweep, k * BLOCKS + b])
            pieces.append(value)
        return jnp.concatenate(pieces, axis=0)

    def col_spread(sweep, value):
        along[sweep, z] = value
        for device in up:
            copy(along.at[sweep, z], along.at[sweep, z], along_sem.at[sweep], device)

    def col_swap(sweep):
        took(along.at[sweep, pl.ds(0, len(up))], along_sem.at[sweep])
        value = along[sweep, 0]
        for d in range(1, NZ):
            value = jnp.maximum(value, along[sweep, d])
        pair_src[sweep] = value
        copy(pair_src.at[sweep], pair_got.at[sweep], pair_sem.at[sweep], partner)

    def col_result(sweep):
        took(pair_got.at[sweep], pair_sem.at[sweep])
        return jnp.maximum(pair_src[sweep], pair_got[sweep])

    def rescale(scale, largest, sweep):
        if sweep == 0:
            return 1.0 / jnp.sqrt(largest)
        return scale / jnp.sqrt((largest * scale) * (1.0 / LIFT))

    def factors(scale, u_ref, v_ref):
        low = jnp.minimum(scale, KNEE)
        u_ref[...] = low * LIFT
        v_ref[...] = scale / low

    def again(source, u_ref, v_ref, from_ref, to_ref, iota, split):
        def body(s, total):
            pick = from_ref[s]
            value = source[s].astype(jnp.float32) * u_ref[pl.ds(pick, 1), :]
            if split:
                value = value * v_ref[pl.ds(pick, 1), :]
            value = jnp.maximum(value[:, :half], value[:, half:])
            value = jnp.max(value.T, axis=0, keepdims=True)
            return put(total, iota, to_ref[s], s, value)

        return lax.fori_loop(0, slots, body, jnp.zeros(iota.shape, jnp.float32), unroll=4)

    def row_pass(split):
        return again(tiles, col_u, col_v, bcol_ref, brow_ref, row_iota, split)

    def col_pass(split):
        return again(turned, row_u, row_v, brow_ref, bcol_ref, col_iota, split)

    pl.semaphore_wait(barrier, len(everyone))
    row_scatter(0, rows)
    col_spread(0, cols)
    row_scale = col_scale = None
    for sweep in range(SWEEPS):
        row_spread(sweep)
        col_swap(sweep)
        new_col = rescale(col_scale, col_result(sweep), sweep)
        last = sweep == SWEEPS - 1
        if not last:
            factors(new_col, col_u, col_v)
            row_scatter(sweep + 1, row_pass(sweep > 0))
        new_row = rescale(row_scale, row_result(sweep), sweep)
        if not last:
            factors(new_row, row_u, row_v)
            col_spread(sweep + 1, col_pass(sweep > 0))
        row_scale, col_scale = new_row, new_col
    row_ref[...] = row_scale
    col_ref[...] = col_scale

    for sweep in range(SWEEPS):
        took(rs_got.at[sweep], send_sem)
        took(plane.at[sweep, pl.ds(0, len(flat))], send_sem)
        took(along.at[sweep, pl.ds(0, len(up))], send_sem)
        took(pair_got.at[sweep], send_sem)


def on_device(tiles, tile_brow, tile_bcol, tile_count):
    slots, width = tiles.shape[2], tiles.shape[3]
    brs = 32
    bcs = brs * (NZ * NC) // (NX * NY)
    piece = brs // PIECES
    f32 = jnp.float32
    smem = pl.BlockSpec(memory_space=pltpu.SMEM)
    vmem = pl.BlockSpec(memory_space=pltpu.VMEM)
    rows, cols = pl.pallas_call(
        kernel,
        out_shape=(
            jax.ShapeDtypeStruct((brs, width), f32),
            jax.ShapeDtypeStruct((bcs, width), f32),
        ),
        in_specs=[smem, smem, smem, pl.BlockSpec(memory_space=pl.ANY)],
        out_specs=(vmem, vmem),
        scratch_shapes=[
            pltpu.VMEM((slots, width, width), jnp.bfloat16),
            pltpu.VMEM((slots, width, width), jnp.bfloat16),
            pltpu.VMEM((brs, width), f32),
            pltpu.VMEM((brs, width), f32),
            pltpu.VMEM((bcs, width), f32),
            pltpu.VMEM((bcs, width), f32),
            pltpu.VMEM((SWEEPS, brs, width), f32),
            pltpu.VMEM((SWEEPS, 3, piece, width), f32),
            pltpu.VMEM((SWEEPS, PIECES * BLOCKS, piece, width), f32),
            pltpu.VMEM((SWEEPS, NZ, bcs, width), f32),
            pltpu.VMEM((SWEEPS, bcs, width), f32),
            pltpu.VMEM((SWEEPS, bcs, width), f32),
            pltpu.SemaphoreType.DMA((slots,)),
            pltpu.SemaphoreType.DMA,
            pltpu.SemaphoreType.DMA((SWEEPS,)),
            pltpu.SemaphoreType.DMA((SWEEPS,)),
            pltpu.SemaphoreType.DMA((SWEEPS,)),
            pltpu.SemaphoreType.DMA((SWEEPS,)),
        ],
        name="equilibrate",
        compiler_params=pltpu.CompilerParams(
            collective_id=0, has_side_effects=True, vmem_limit_bytes=32 * 1024 * 1024
        ),
    )(
        tile_count.reshape(1),
        tile_brow.reshape(slots),
        tile_bcol.reshape(slots),
        tiles.reshape(slots, width, width),
    )
    return rows.reshape(brs, 1, width), cols.reshape(bcs, 1, width)


def solution(mesh):
    in_specs = (
        P("prow", "pcol", None, None, None),
        P("prow", "pcol", None),
        P("prow", "pcol", None),
        P("prow", "pcol"),
    )
    out_specs = (P(None, "prow", None), P(None, "pcol", None))
    return jax.shard_map(
        on_device, mesh=mesh, in_specs=in_specs, out_specs=out_specs, check_vma=False
    )
```

```python
import functools

import jax
import jax.numpy as jnp
from jax import lax
from jax.experimental import pallas as pl
from jax.experimental.pallas import tpu as pltpu
from jax.sharding import PartitionSpec as P

MESH = pl.DeviceIdType.MESH
SWEEPS = 3
NX, NY, NZ, NC = 4, 8, 8, 2
PIECES, BLOCKS = 8, 4
REACH = 2
CHUNK = 4
VMEM_LIMIT = 32 * 1024 * 1024
UNROLL = 16
LIFT = 2.0**63
KNEE = 2.0**64


def kernel(
    count_ref, brow_hbm, bcol_hbm, tiles_hbm, row_ref, col_ref,
    brow_smem, bcol_smem, tiles, turned, row_u, row_v, col_u, col_v,
    rs_src, rs_got, plane, along, pair_src, pair_got,
    enter_sem, index_sem, load_sem, send_sem, rs_sem, plane_sem, along_sem, pair_sem,
):
    slots, width = tiles.shape[0], tiles.shape[1]
    half = width // 2
    brs, bcs = row_ref.shape[0], col_ref.shape[0]
    piece = brs * 2 // PIECES
    prow, pcol = lax.axis_index("prow"), lax.axis_index("pcol")
    z, core = prow // NC, prow % NC
    y, x = pcol // NX, pcol % NX
    part = (y % 2) * NX + x
    block = y // 2
    mine = part * BLOCKS + block

    indices = [
        pltpu.make_async_copy(src, dst, index_sem.at[i])
        for i, (src, dst) in enumerate(
            ((brow_hbm, brow_smem), (bcol_hbm, bcol_smem))
        )
    ]
    loads = [
        pltpu.make_async_copy(
            tiles_hbm.at[0, 0, pl.ds(c * CHUNK, CHUNK)],
            tiles.at[pl.ds(c * CHUNK, CHUNK)], load_sem.at[c],
        )
        for c in range(slots // CHUNK)
    ]
    for load in loads + indices:
        load.start()

    near = []
    for d in range(1, PIECES):
        px = lax.rem(x + d, NX)
        py = y + (1 - 2 * (y % 2)) * (d // NX)
        near.append(((py % 2) * NX + px, (prow, py * NX + px)))
    beyond = [(prow, lax.rem(y + d, NY) * NX + x) for d in (REACH, NY - REACH)]
    offsets = [(dy, dx) for dy in range(NY) for dx in range(NX) if (dy, dx) != (0, 0)]
    offsets.sort(key=lambda o: -(min(o[0], NY - o[0]) + min(o[1], NX - o[1])))
    flat = [
        (prow, lax.rem(y + dy, NY) * NX + lax.rem(x + dx, NX)) for dy, dx in offsets
    ]
    steps = sorted(range(1, NZ), key=lambda d: -min(d, NZ - d))
    up = [(lax.rem(z + d, NZ) * NC + core, pcol) for d in steps]
    partner = (z * NC + 1 - core, pcol)

    barrier = pltpu.get_barrier_semaphore()
    everyone = [device for _, device in near] + beyond + up + [partner]
    for device in everyone:
        pl.semaphore_signal(barrier, inc=1, device_id=device, device_id_type=MESH)

    with jax.named_scope("index"):
        for load in indices:
            load.wait()
    count = count_ref[0]
    brow_ref, bcol_ref = brow_smem.at[0, 0], bcol_smem.at[0, 0]
    row_iota = lax.broadcasted_iota(jnp.int32, (brs, width), 0)
    col_iota = lax.broadcasted_iota(jnp.int32, (bcs, width), 0)

    def put(total, iota, where_to, s, value):
        place = jnp.where(s < count, where_to, -1)
        return jnp.maximum(total, jnp.where(iota == place, value, 0.0))

    def first(c, totals):
        rows, cols = totals
        pltpu.make_async_copy(
            tiles_hbm.at[0, 0, pl.ds(c * CHUNK, CHUNK)],
            tiles.at[pl.ds(c * CHUNK, CHUNK)], load_sem.at[c],
        ).wait()
        for i in range(CHUNK):
            s = c * CHUNK + i
            tile = jnp.abs(tiles[s])
            tiles[s] = tile
            fold = jnp.maximum(tile[:, :half], tile[:, half:]).T
            row = jnp.max(fold, axis=0, keepdims=True).astype(jnp.float32)
            col = jnp.max(tile, axis=0, keepdims=True).astype(jnp.float32)
            rows = put(rows, row_iota, brow_ref[s], s, row)
            cols = put(cols, col_iota, bcol_ref[s], s, col)
        return rows, cols

    totals = (jnp.zeros((brs, width), jnp.float32), jnp.zeros((bcs, width), jnp.float32))
    with jax.named_scope("first"):
        rows, cols = lax.fori_loop(0, slots // CHUNK, first, totals)

    def turn(s, _):
        turned[s] = tiles[s].T
        return 0

    def copy(src, dst, sem, device):
        pltpu.make_async_remote_copy(
            src_ref=src, dst_ref=dst, send_sem=send_sem, recv_sem=sem,
            device_id=device, device_id_type=MESH,
        ).start()

    def took(ref, sem):
        pltpu.make_async_copy(ref, ref, sem).wait()

    def spot(k):
        return (
            pl.ds(pl.multiple_of(k // 2 * piece, piece), piece),
            pl.ds(pl.multiple_of(k % 2 * half, half), half),
        )

    def row_scatter(sweep, value):
        rs_src[sweep] = value
        for d, (k, device) in enumerate(near):
            copy(rs_src.at[(sweep, *spot(k))], rs_got.at[sweep, d], rs_sem.at[sweep], device)

    def row_spread(sweep):
        with jax.named_scope("rs_wait"):
            took(rs_got.at[sweep], rs_sem.at[sweep])
        value = rs_src[(sweep, *spot(part))]
        for d in range(len(near)):
            value = jnp.maximum(value, rs_got[sweep, d])
        plane[sweep, mine] = value
        for device in flat:
            copy(plane.at[sweep, mine], plane.at[sweep, mine], plane_sem.at[sweep], device)

    def row_result(sweep):
        with jax.named_scope("plane_wait"):
            took(plane.at[sweep, pl.ds(0, len(flat))], plane_sem.at[sweep])
        pieces = []
        for k in range(PIECES):
            value = plane[sweep, k * BLOCKS]
            for b in range(1, BLOCKS):
                value = jnp.maximum(value, plane[sweep, k * BLOCKS + b])
            pieces.append(value)
        return jnp.concatenate(
            [jnp.concatenate(pieces[k : k + 2], axis=1) for k in range(0, PIECES, 2)],
            axis=0,
        )

    def col_spread(sweep, value):
        along[sweep, z] = value
        for device in up:
            copy(along.at[sweep, z], along.at[sweep, z], along_sem.at[sweep], device)

    def col_swap(sweep):
        with jax.named_scope("along_wait"):
            took(along.at[sweep, pl.ds(0, len(up))], along_sem.at[sweep])
        value = along[sweep, 0]
        for d in range(1, NZ):
            value = jnp.maximum(value, along[sweep, d])
        pair_src[sweep] = value
        copy(pair_src.at[sweep], pair_got.at[sweep], pair_sem.at[sweep], partner)

    def col_result(sweep):
        with jax.named_scope("pair_wait"):
            took(pair_got.at[sweep], pair_sem.at[sweep])
        return jnp.maximum(pair_src[sweep], pair_got[sweep])

    def rescale(scale, largest, sweep):
        if sweep == 0:
            return 1.0 / jnp.sqrt(largest)
        return scale / jnp.sqrt((largest * scale) * (1.0 / LIFT))

    def factors(scale, u_ref, v_ref):
        low = jnp.minimum(scale, KNEE)
        u_ref[...] = low * LIFT
        v_ref[...] = scale / low

    def again(source, u_ref, v_ref, from_ref, to_ref, iota, split):
        def body(s, total):
            pick = from_ref[s]
            value = source[s].astype(jnp.float32) * u_ref[pl.ds(pick, 1), :]
            if split:
                value = value * v_ref[pl.ds(pick, 1), :]
            value = jnp.maximum(value[:, :half], value[:, half:])
            value = jnp.max(value.T, axis=0, keepdims=True)
            return put(total, iota, to_ref[s], s, value)

        return lax.fori_loop(0, slots, body, jnp.zeros(iota.shape, jnp.float32), unroll=UNROLL)

    def row_pass(split):
        return again(tiles, col_u, col_v, bcol_ref, brow_ref, row_iota, split)

    def col_pass(split):
        return again(turned, row_u, row_v, brow_ref, bcol_ref, col_iota, split)

    with jax.named_scope("enter"):
        pl.semaphore_wait(barrier, len(everyone))
    row_scatter(0, rows)
    col_spread(0, cols)
    for stage in range(2):
        for device in beyond:
            pl.semaphore_signal(
                enter_sem.at[stage], inc=1, device_id=device, device_id_type=MESH
            )
        with jax.named_scope("turn"):
            lax.fori_loop(stage * slots // 2, (stage + 1) * slots // 2, turn, 0, unroll=8)
        with jax.named_scope("stage"):
            pl.semaphore_wait(enter_sem.at[stage], len(beyond))
    row_scale = col_scale = None
    for sweep in range(SWEEPS):
        row_spread(sweep)
        col_swap(sweep)
        new_col = rescale(col_scale, col_result(sweep), sweep)
        last = sweep == SWEEPS - 1
        if not last:
            factors(new_col, col_u, col_v)
            with jax.named_scope("row_pass"):
                value = row_pass(sweep > 0)
            row_scatter(sweep + 1, value)
        new_row = rescale(row_scale, row_result(sweep), sweep)
        if not last:
            factors(new_row, row_u, row_v)
            with jax.named_scope("col_pass"):
                value = col_pass(sweep > 0)
            col_spread(sweep + 1, value)
        row_scale, col_scale = new_row, new_col
    row_ref[...] = row_scale.reshape(row_ref.shape)
    col_ref[...] = col_scale.reshape(col_ref.shape)

    with jax.named_scope("drain"):
        for sweep in range(SWEEPS):
            took(rs_got.at[sweep], send_sem)
            took(plane.at[sweep, pl.ds(0, len(flat))], send_sem)
            took(along.at[sweep, pl.ds(0, len(up))], send_sem)
            took(pair_got.at[sweep], send_sem)


def finish(rows, cols, row_ref, col_ref):
    row_ref[...] = rows[...]
    col_ref[...] = cols[...]


def on_device(tiles, tile_brow, tile_bcol, tile_count):
    slots, width = tiles.shape[2], tiles.shape[3]
    brs = 32
    bcs = brs * (NZ * NC) // (NX * NY)
    piece, half = brs * 2 // PIECES, width // 2
    f32 = jnp.float32
    vmem = pl.BlockSpec(memory_space=pltpu.VMEM)
    rows, cols = pl.pallas_call(
        kernel,
        out_shape=(
            jax.ShapeDtypeStruct((brs, 1, width), f32),
            jax.ShapeDtypeStruct((bcs, 1, width), f32),
        ),
        in_specs=[pl.BlockSpec(memory_space=pltpu.SMEM)] + [pl.BlockSpec(memory_space=pltpu.HBM)] * 3,
        out_specs=(vmem, vmem),
        scratch_shapes=[
            pltpu.SMEM((1, 1, slots), jnp.int32),
            pltpu.SMEM((1, 1, slots), jnp.int32),
            pltpu.VMEM((slots, width, width), jnp.bfloat16),
            pltpu.VMEM((slots, width, width), jnp.bfloat16),
            pltpu.VMEM((brs, width), f32),
            pltpu.VMEM((brs, width), f32),
            pltpu.VMEM((bcs, width), f32),
            pltpu.VMEM((bcs, width), f32),
            pltpu.VMEM((SWEEPS, brs, width), f32),
            pltpu.VMEM((SWEEPS, PIECES - 1, piece, half), f32),
            pltpu.VMEM((SWEEPS, PIECES * BLOCKS, piece, half), f32),
            pltpu.VMEM((SWEEPS, NZ, bcs, width), f32),
            pltpu.VMEM((SWEEPS, bcs, width), f32),
            pltpu.VMEM((SWEEPS, bcs, width), f32),
            pltpu.SemaphoreType.REGULAR((2,)),
            pltpu.SemaphoreType.DMA((2,)),
            pltpu.SemaphoreType.DMA((slots // CHUNK,)),
            pltpu.SemaphoreType.DMA,
            pltpu.SemaphoreType.DMA((SWEEPS,)),
            pltpu.SemaphoreType.DMA((SWEEPS,)),
            pltpu.SemaphoreType.DMA((SWEEPS,)),
            pltpu.SemaphoreType.DMA((SWEEPS,)),
        ],
        name="equilibrate",
        compiler_params=pltpu.CompilerParams(
            collective_id=0, has_side_effects=True, vmem_limit_bytes=VMEM_LIMIT
        ),
    )(
        tile_count.reshape(1),
        *(
            pltpu.with_memory_space_constraint(a, pltpu.HBM)
            for a in (tile_brow, tile_bcol, tiles)
        ),
    )
    return rows, cols
    return pl.pallas_call(
        finish,
        out_shape=(
            jax.ShapeDtypeStruct(rows.shape, f32),
            jax.ShapeDtypeStruct(cols.shape, f32),
        ),
        in_specs=[vmem, vmem],
        out_specs=(vmem, vmem),
        name="finish",
    )(rows, cols)


def solution(mesh):
    in_specs = (
        P("prow", "pcol", None, None, None),
        P("prow", "pcol", None),
        P("prow", "pcol", None),
        P("prow", "pcol"),
    )
    out_specs = (P(None, "prow", None), P(None, "pcol", None))
    return jax.shard_map(
        on_device, mesh=mesh, in_specs=in_specs, out_specs=out_specs, check_vma=False
    )
```

```python
import functools

import jax
import jax.numpy as jnp
from jax import lax
from jax.experimental import pallas as pl
from jax.experimental.pallas import tpu as pltpu
from jax.sharding import PartitionSpec as P

MESH = pl.DeviceIdType.MESH
SWEEPS = 3
NX, NY, NZ, NC = 4, 8, 8, 2
PIECES, BLOCKS = 8, 4
REACHES = (1, 2)
CHUNK = 4
VMEM_LIMIT = 32 * 1024 * 1024
UNROLL = 32
LIFT = 2.0**63
KNEE = 2.0**64


def kernel(
    count_ref, brow_hbm, bcol_hbm, tiles_hbm, row_ref, col_ref,
    brow_smem, bcol_smem, tiles, turned, row_u, row_v, col_u, col_v,
    rs_src, rs_got, plane, along, pair_src, pair_got,
    enter_sem, index_sem, load_sem, send_sem, rs_sem, plane_sem, along_sem, pair_sem,
):
    slots, width = tiles.shape[0], tiles.shape[1]
    half = width // 2
    brs, bcs = row_ref.shape[0], col_ref.shape[0]
    piece = brs * 2 // PIECES
    prow, pcol = lax.axis_index("prow"), lax.axis_index("pcol")
    z, core = prow // NC, prow % NC
    y, x = pcol // NX, pcol % NX
    part = (y % 2) * NX + x
    block = y // 2
    mine = part * BLOCKS + block

    indices = [
        pltpu.make_async_copy(src, dst, index_sem.at[i])
        for i, (src, dst) in enumerate(
            ((brow_hbm, brow_smem), (bcol_hbm, bcol_smem))
        )
    ]
    loads = [
        pltpu.make_async_copy(
            tiles_hbm.at[0, 0, pl.ds(c * CHUNK, CHUNK)],
            tiles.at[pl.ds(c * CHUNK, CHUNK)], load_sem.at[c],
        )
        for c in range(slots // CHUNK)
    ]
    for load in loads + indices:
        load.start()

    near = []
    for d in range(1, PIECES):
        px = lax.rem(x + d, NX)
        py = y + (1 - 2 * (y % 2)) * (d // NX)
        near.append(((py % 2) * NX + px, (prow, py * NX + px)))
    greet = [
        (prow, lax.rem(y + dy, NY) * NX + lax.rem(x + dx, NX))
        for dy in (1, NY - 1, 0) for dx in range(NX) if (dy, dx) != (0, 0)
    ]
    beyond = [
        [(prow, lax.rem(y + d, NY) * NX + x) for d in (reach, NY - reach)]
        for reach in REACHES
    ]
    offsets = [(dy, dx) for dy in range(NY) for dx in range(NX) if (dy, dx) != (0, 0)]
    offsets.sort(key=lambda o: -(min(o[0], NY - o[0]) + min(o[1], NX - o[1])))
    flat = [
        (prow, lax.rem(y + dy, NY) * NX + lax.rem(x + dx, NX)) for dy, dx in offsets
    ]
    steps = sorted(range(1, NZ), key=lambda d: -min(d, NZ - d))
    up = [(lax.rem(z + d, NZ) * NC + core, pcol) for d in steps]
    partner = (z * NC + 1 - core, pcol)

    barrier = pltpu.get_barrier_semaphore()
    everyone = greet + up + [partner]
    for device in everyone:
        pl.semaphore_signal(barrier, inc=1, device_id=device, device_id_type=MESH)

    with jax.named_scope("index"):
        for load in indices:
            load.wait()
    count = count_ref[0]
    brow_ref, bcol_ref = brow_smem.at[0, 0], bcol_smem.at[0, 0]
    row_iota = lax.broadcasted_iota(jnp.int32, (brs, width), 0)
    col_iota = lax.broadcasted_iota(jnp.int32, (bcs, width), 0)

    def put(total, iota, where_to, s, value):
        place = jnp.where(s < count, where_to, -1)
        return jnp.maximum(total, jnp.where(iota == place, value, 0.0))

    def first(c, totals):
        rows, cols = totals
        pltpu.make_async_copy(
            tiles_hbm.at[0, 0, pl.ds(c * CHUNK, CHUNK)],
            tiles.at[pl.ds(c * CHUNK, CHUNK)], load_sem.at[c],
        ).wait()
        for i in range(CHUNK):
            s = c * CHUNK + i
            tile = jnp.abs(tiles[s])
            tiles[s] = tile
            fold = jnp.maximum(tile[:, :half], tile[:, half:]).T
            row = jnp.max(fold, axis=0, keepdims=True).astype(jnp.float32)
            col = jnp.max(tile, axis=0, keepdims=True).astype(jnp.float32)
            rows = put(rows, row_iota, brow_ref[s], s, row)
            cols = put(cols, col_iota, bcol_ref[s], s, col)
        return rows, cols

    totals = (jnp.zeros((brs, width), jnp.float32), jnp.zeros((bcs, width), jnp.float32))
    with jax.named_scope("first"):
        rows, cols = lax.fori_loop(0, slots // CHUNK, first, totals)

    def turn(s, _):
        turned[s] = tiles[s].T
        return 0

    def copy(src, dst, sem, device):
        pltpu.make_async_remote_copy(
            src_ref=src, dst_ref=dst, send_sem=send_sem, recv_sem=sem,
            device_id=device, device_id_type=MESH,
        ).start()

    def took(ref, sem):
        pltpu.make_async_copy(ref, ref, sem).wait()

    def spot(k):
        return (
            pl.ds(pl.multiple_of(k // 2 * piece, piece), piece),
            pl.ds(pl.multiple_of(k % 2 * half, half), half),
        )

    def row_scatter(sweep, value):
        rs_src[sweep] = value
        for d, (k, device) in enumerate(near):
            copy(rs_src.at[(sweep, *spot(k))], rs_got.at[sweep, d], rs_sem.at[sweep], device)

    def row_spread(sweep):
        with jax.named_scope("rs_wait"):
            took(rs_got.at[sweep], rs_sem.at[sweep])
        value = rs_src[(sweep, *spot(part))]
        for d in range(len(near)):
            value = jnp.maximum(value, rs_got[sweep, d])
        plane[sweep, mine] = value
        for device in flat:
            copy(plane.at[sweep, mine], plane.at[sweep, mine], plane_sem.at[sweep], device)

    def row_result(sweep):
        with jax.named_scope("plane_wait"):
            took(plane.at[sweep, pl.ds(0, len(flat))], plane_sem.at[sweep])
        pieces = []
        for k in range(PIECES):
            value = plane[sweep, k * BLOCKS]
            for b in range(1, BLOCKS):
                value = jnp.maximum(value, plane[sweep, k * BLOCKS + b])
            pieces.append(value)
        return jnp.concatenate(
            [jnp.concatenate(pieces[k : k + 2], axis=1) for k in range(0, PIECES, 2)],
            axis=0,
        )

    def col_spread(sweep, value):
        along[sweep, z] = value
        for device in up:
            copy(along.at[sweep, z], along.at[sweep, z], along_sem.at[sweep], device)

    def col_swap(sweep):
        with jax.named_scope("along_wait"):
            took(along.at[sweep, pl.ds(0, len(up))], along_sem.at[sweep])
        value = along[sweep, 0]
        for d in range(1, NZ):
            value = jnp.maximum(value, along[sweep, d])
        pair_src[sweep] = value
        copy(pair_src.at[sweep], pair_got.at[sweep], pair_sem.at[sweep], partner)

    def col_result(sweep):
        with jax.named_scope("pair_wait"):
            took(pair_got.at[sweep], pair_sem.at[sweep])
        return jnp.maximum(pair_src[sweep], pair_got[sweep])

    def rescale(scale, largest, sweep):
        if sweep == 0:
            return 1.0 / jnp.sqrt(largest)
        return scale / jnp.sqrt((largest * scale) * (1.0 / LIFT))

    def factors(scale, u_ref, v_ref):
        low = jnp.minimum(scale, KNEE)
        u_ref[...] = low * LIFT
        v_ref[...] = scale / low

    def again(source, u_ref, v_ref, from_ref, to_ref, iota, split):
        def body(s, total):
            pick = from_ref[s]
            value = source[s].astype(jnp.float32) * u_ref[pl.ds(pick, 1), :]
            if split:
                value = value * v_ref[pl.ds(pick, 1), :]
            value = jnp.maximum(value[:, :half], value[:, half:])
            value = jnp.max(value.T, axis=0, keepdims=True)
            return put(total, iota, to_ref[s], s, value)

        return lax.fori_loop(0, slots, body, jnp.zeros(iota.shape, jnp.float32), unroll=UNROLL)

    def row_pass(split):
        return again(tiles, col_u, col_v, bcol_ref, brow_ref, row_iota, split)

    def col_pass(split):
        return again(turned, row_u, row_v, brow_ref, bcol_ref, col_iota, split)

    with jax.named_scope("enter"):
        pl.semaphore_wait(barrier, len(everyone))
    row_scatter(0, rows)
    col_spread(0, cols)
    for stage, devices in enumerate(beyond):
        for device in devices:
            pl.semaphore_signal(
                enter_sem.at[stage], inc=1, device_id=device, device_id_type=MESH
            )
        if stage == len(beyond) - 1:
            with jax.named_scope("turn"):
                lax.fori_loop(0, slots, turn, 0, unroll=8)
        with jax.named_scope("stage"):
            pl.semaphore_wait(enter_sem.at[stage], len(devices))
    row_scale = col_scale = None
    for sweep in range(SWEEPS):
        row_spread(sweep)
        col_swap(sweep)
        new_col = rescale(col_scale, col_result(sweep), sweep)
        last = sweep == SWEEPS - 1
        if not last:
            factors(new_col, col_u, col_v)
            with jax.named_scope("row_pass"):
                value = row_pass(sweep > 0)
            row_scatter(sweep + 1, value)
        new_row = rescale(row_scale, row_result(sweep), sweep)
        if not last:
            factors(new_row, row_u, row_v)
            with jax.named_scope("col_pass"):
                value = col_pass(sweep > 0)
            col_spread(sweep + 1, value)
        row_scale, col_scale = new_row, new_col
    row_ref[...] = row_scale.reshape(row_ref.shape)
    col_ref[...] = col_scale.reshape(col_ref.shape)

    with jax.named_scope("drain"):
        for sweep in range(SWEEPS):
            took(rs_got.at[sweep], send_sem)
            took(plane.at[sweep, pl.ds(0, len(flat))], send_sem)
            took(along.at[sweep, pl.ds(0, len(up))], send_sem)
            took(pair_got.at[sweep], send_sem)


def finish(rows, cols, row_out, col_out, sem):
    moves = [
        pltpu.make_async_copy(src, dst, sem.at[i])
        for i, (src, dst) in enumerate(((rows, row_out), (cols, col_out)))
    ]
    for move in moves:
        move.start()
    for move in moves:
        move.wait()


def on_device(tiles, tile_brow, tile_bcol, tile_count):
    slots, width = tiles.shape[2], tiles.shape[3]
    brs = 32
    bcs = brs * (NZ * NC) // (NX * NY)
    piece, half = brs * 2 // PIECES, width // 2
    f32 = jnp.float32
    vmem = pl.BlockSpec(memory_space=pltpu.VMEM)
    rows, cols = pl.pallas_call(
        kernel,
        out_shape=(
            jax.ShapeDtypeStruct((brs, 1, width), f32),
            jax.ShapeDtypeStruct((bcs, 1, width), f32),
        ),
        in_specs=[pl.BlockSpec(memory_space=pltpu.SMEM)] + [pl.BlockSpec(memory_space=pltpu.HBM)] * 3,
        out_specs=(vmem, vmem),
        scratch_shapes=[
            pltpu.SMEM((1, 1, slots), jnp.int32),
            pltpu.SMEM((1, 1, slots), jnp.int32),
            pltpu.VMEM((slots, width, width), jnp.bfloat16),
            pltpu.VMEM((slots, width, width), jnp.bfloat16),
            pltpu.VMEM((brs, width), f32),
            pltpu.VMEM((brs, width), f32),
            pltpu.VMEM((bcs, width), f32),
            pltpu.VMEM((bcs, width), f32),
            pltpu.VMEM((SWEEPS, brs, width), f32),
            pltpu.VMEM((SWEEPS, PIECES - 1, piece, half), f32),
            pltpu.VMEM((SWEEPS, PIECES * BLOCKS, piece, half), f32),
            pltpu.VMEM((SWEEPS, NZ, bcs, width), f32),
            pltpu.VMEM((SWEEPS, bcs, width), f32),
            pltpu.VMEM((SWEEPS, bcs, width), f32),
            pltpu.SemaphoreType.REGULAR((2,)),
            pltpu.SemaphoreType.DMA((2,)),
            pltpu.SemaphoreType.DMA((slots // CHUNK,)),
            pltpu.SemaphoreType.DMA,
            pltpu.SemaphoreType.DMA((SWEEPS,)),
            pltpu.SemaphoreType.DMA((SWEEPS,)),
            pltpu.SemaphoreType.DMA((SWEEPS,)),
            pltpu.SemaphoreType.DMA((SWEEPS,)),
        ],
        name="equilibrate",
        compiler_params=pltpu.CompilerParams(
            collective_id=0, has_side_effects=True, vmem_limit_bytes=VMEM_LIMIT
        ),
    )(
        tile_count.reshape(1),
        *(
            pltpu.with_memory_space_constraint(a, pltpu.HBM)
            for a in (tile_brow, tile_bcol, tiles)
        ),
    )
    anywhere = pl.BlockSpec(memory_space=pltpu.HBM)
    return pl.pallas_call(
        finish,
        out_shape=(
            jax.ShapeDtypeStruct(rows.shape, f32),
            jax.ShapeDtypeStruct(cols.shape, f32),
        ),
        in_specs=[vmem, vmem],
        out_specs=(anywhere, anywhere),
        scratch_shapes=[pltpu.SemaphoreType.DMA((2,))],
        name="finish",
    )(*(pltpu.with_memory_space_constraint(a, pltpu.VMEM) for a in (rows, cols)))


def solution(mesh):
    in_specs = (
        P("prow", "pcol", None, None, None),
        P("prow", "pcol", None),
        P("prow", "pcol", None),
        P("prow", "pcol"),
    )
    out_specs = (P(None, "prow", None), P(None, "pcol", None))
    return jax.shard_map(
        on_device, mesh=mesh, in_specs=in_specs, out_specs=out_specs, check_vma=False
    )
```

```python
import functools

import jax
import jax.numpy as jnp
from jax import lax
from jax.experimental import pallas as pl
from jax.experimental.pallas import tpu as pltpu
from jax.sharding import PartitionSpec as P

MESH = pl.DeviceIdType.MESH
SWEEPS = 3
NX, NY, NZ, NC = 4, 8, 8, 2
PAIRS = 4
APART = (0, 1, 1, 2)
REACHES = (1, 2)
CHUNK = 4
VMEM_LIMIT = 32 * 1024 * 1024
UNROLL = 32
LIFT = 2.0**63
KNEE = 2.0**64


def kernel(
    count_ref, brow_hbm, bcol_hbm, tiles_hbm, row_ref, col_ref,
    brow_smem, bcol_smem, tiles, turned, row_u, row_v, col_u, col_v,
    rs_src, rs_got, plane, along, pair_src, pair_got,
    enter_sem, index_sem, load_sem, send_sem, rs_sem, plane_sem, along_sem, pair_sem,
):
    slots, width = tiles.shape[0], tiles.shape[1]
    half = width // 2
    brs, bcs = row_ref.shape[0], col_ref.shape[0]
    piece = brs // NX
    prow, pcol = lax.axis_index("prow"), lax.axis_index("pcol")
    z, core = prow // NC, prow % NC
    y, x = pcol // NX, pcol % NX

    indices = [
        pltpu.make_async_copy(src, dst, index_sem.at[i])
        for i, (src, dst) in enumerate(
            ((brow_hbm, brow_smem), (bcol_hbm, bcol_smem))
        )
    ]
    loads = [
        pltpu.make_async_copy(
            tiles_hbm.at[0, 0, pl.ds(c * CHUNK, CHUNK)],
            tiles.at[pl.ds(c * CHUNK, CHUNK)], load_sem.at[c],
        )
        for c in range(slots // CHUNK)
    ]
    for load in loads + indices:
        load.start()

    side = 2 * (y % 2) - 1
    near, far = [], []
    for turns in (1, 0):
        for dx in (2, 1, 3, 0):
            if (turns, dx) != (0, 0):
                px = lax.rem(x + dx, NX)
                near.append((px, (prow, (y - side * turns) * NX + px)))
    for turns in (3, 2, 1, 0):
        for dx in (2, 1, 3, 0):
            if (turns, dx) != (0, 0):
                py = lax.rem(y + NY + side * turns, NY)
                slot = lax.rem(PAIRS - side * APART[turns], PAIRS)
                far.append((slot, (prow, py * NX + lax.rem(x + dx, NX))))
    greet = [
        (prow, lax.rem(y + dy, NY) * NX + lax.rem(x + dx, NX))
        for dy in (1, NY - 1, 0) for dx in range(NX) if (dy, dx) != (0, 0)
    ]
    beyond = [
        [(prow, lax.rem(y + d, NY) * NX + x) for d in (reach, NY - reach)]
        for reach in REACHES
    ]
    steps = sorted(range(1, NZ), key=lambda d: -min(d, NZ - d))
    up = [(lax.rem(z + d, NZ) * NC + core, pcol) for d in steps]
    partner = (z * NC + 1 - core, pcol)

    barrier = pltpu.get_barrier_semaphore()
    everyone = greet + up + [partner]
    for device in everyone:
        pl.semaphore_signal(barrier, inc=1, device_id=device, device_id_type=MESH)

    with jax.named_scope("index"):
        for load in indices:
            load.wait()
    count = count_ref[0]
    brow_ref, bcol_ref = brow_smem.at[0, 0], bcol_smem.at[0, 0]
    row_iota = lax.broadcasted_iota(jnp.int32, (brs, width), 0)
    col_iota = lax.broadcasted_iota(jnp.int32, (bcs, width), 0)

    def put(total, iota, where_to, s, value):
        place = jnp.where(s < count, where_to, -1)
        return jnp.maximum(total, jnp.where(iota == place, value, 0.0))

    def first(c, totals):
        rows, cols = totals
        pltpu.make_async_copy(
            tiles_hbm.at[0, 0, pl.ds(c * CHUNK, CHUNK)],
            tiles.at[pl.ds(c * CHUNK, CHUNK)], load_sem.at[c],
        ).wait()
        for i in range(CHUNK):
            s = c * CHUNK + i
            tile = jnp.abs(tiles[s])
            tiles[s] = tile
            fold = jnp.maximum(tile[:, :half], tile[:, half:]).T
            row = jnp.max(fold, axis=0, keepdims=True).astype(jnp.float32)
            col = jnp.max(tile, axis=0, keepdims=True).astype(jnp.float32)
            rows = put(rows, row_iota, brow_ref[s], s, row)
            cols = put(cols, col_iota, bcol_ref[s], s, col)
        return rows, cols

    totals = (jnp.zeros((brs, width), jnp.float32), jnp.zeros((bcs, width), jnp.float32))
    with jax.named_scope("first"):
        rows, cols = lax.fori_loop(0, slots // CHUNK, first, totals)

    def turn(s, _):
        turned[s] = tiles[s].T
        return 0

    def copy(src, dst, sem, device):
        pltpu.make_async_remote_copy(
            src_ref=src, dst_ref=dst, send_sem=send_sem, recv_sem=sem,
            device_id=device, device_id_type=MESH,
        ).start()

    def took(ref, sem):
        pltpu.make_async_copy(ref, ref, sem).wait()

    def spot(k):
        return pl.ds(pl.multiple_of(k * piece, piece), piece)

    def row_scatter(sweep, value):
        rs_src[sweep] = value
        for d, (k, device) in enumerate(near):
            copy(rs_src.at[sweep, spot(k)], rs_got.at[sweep, d], rs_sem.at[sweep], device)

    def row_spread(sweep):
        with jax.named_scope("rs_wait"):
            took(rs_got.at[sweep], rs_sem.at[sweep])
        value = rs_src[sweep, spot(x)]
        for d in range(len(near)):
            value = jnp.maximum(value, rs_got[sweep, d])
        plane[sweep, x] = value
        for slot, device in far:
            copy(plane.at[sweep, x], plane.at[sweep, slot * NX + x], plane_sem.at[sweep], device)

    def row_result(sweep):
        with jax.named_scope("plane_wait"):
            took(plane.at[sweep, pl.ds(0, len(far))], plane_sem.at[sweep])
        pieces = []
        for k in range(NX):
            value = plane[sweep, k]
            for b in range(1, PAIRS):
                value = jnp.maximum(value, plane[sweep, b * NX + k])
            pieces.append(value)
        return jnp.concatenate(pieces, axis=0)

    def col_spread(sweep, value):
        along[sweep, z] = value
        for device in up:
            copy(along.at[sweep, z], along.at[sweep, z], along_sem.at[sweep], device)

    def col_swap(sweep):
        with jax.named_scope("along_wait"):
            took(along.at[sweep, pl.ds(0, len(up))], along_sem.at[sweep])
        value = along[sweep, 0]
        for d in range(1, NZ):
            value = jnp.maximum(value, along[sweep, d])
        pair_src[sweep] = value
        copy(pair_src.at[sweep], pair_got.at[sweep], pair_sem.at[sweep], partner)

    def col_result(sweep):
        with jax.named_scope("pair_wait"):
            took(pair_got.at[sweep], pair_sem.at[sweep])
        return jnp.maximum(pair_src[sweep], pair_got[sweep])

    def rescale(scale, largest, sweep):
        if sweep == 0:
            return 1.0 / jnp.sqrt(largest)
        return scale / jnp.sqrt((largest * scale) * (1.0 / LIFT))

    def factors(scale, u_ref, v_ref):
        low = jnp.minimum(scale, KNEE)
        u_ref[...] = low * LIFT
        v_ref[...] = scale / low

    def again(source, u_ref, v_ref, from_ref, to_ref, iota, split):
        def body(s, total):
            pick = from_ref[s]
            value = source[s].astype(jnp.float32) * u_ref[pl.ds(pick, 1), :]
            if split:
                value = value * v_ref[pl.ds(pick, 1), :]
            value = jnp.maximum(value[:, :half], value[:, half:])
            value = jnp.max(value.T, axis=0, keepdims=True)
            return put(total, iota, to_ref[s], s, value)

        return lax.fori_loop(0, slots, body, jnp.zeros(iota.shape, jnp.float32), unroll=UNROLL)

    def row_pass(split):
        return again(tiles, col_u, col_v, bcol_ref, brow_ref, row_iota, split)

    def col_pass(split):
        return again(turned, row_u, row_v, brow_ref, bcol_ref, col_iota, split)

    with jax.named_scope("enter"):
        pl.semaphore_wait(barrier, len(everyone))
    row_scatter(0, rows)
    col_spread(0, cols)
    for stage, devices in enumerate(beyond):
        for device in devices:
            pl.semaphore_signal(
                enter_sem.at[stage], inc=1, device_id=device, device_id_type=MESH
            )
        if stage == len(beyond) - 1:
            with jax.named_scope("turn"):
                lax.fori_loop(0, slots, turn, 0, unroll=8)
        with jax.named_scope("stage"):
            pl.semaphore_wait(enter_sem.at[stage], len(devices))
    row_scale = col_scale = None
    for sweep in range(SWEEPS):
        row_spread(sweep)
        col_swap(sweep)
        new_col = rescale(col_scale, col_result(sweep), sweep)
        last = sweep == SWEEPS - 1
        if not last:
            factors(new_col, col_u, col_v)
            with jax.named_scope("row_pass"):
                value = row_pass(sweep > 0)
            row_scatter(sweep + 1, value)
        new_row = rescale(row_scale, row_result(sweep), sweep)
        if not last:
            factors(new_row, row_u, row_v)
            with jax.named_scope("col_pass"):
                value = col_pass(sweep > 0)
            col_spread(sweep + 1, value)
        row_scale, col_scale = new_row, new_col
    row_ref[...] = row_scale.reshape(row_ref.shape)
    col_ref[...] = col_scale.reshape(col_ref.shape)

    with jax.named_scope("drain"):
        for sweep in range(SWEEPS):
            took(rs_got.at[sweep], send_sem)
            took(plane.at[sweep, pl.ds(0, len(far))], send_sem)
            took(along.at[sweep, pl.ds(0, len(up))], send_sem)
            took(pair_got.at[sweep], send_sem)


def finish(rows, cols, row_out, col_out, sem):
    moves = [
        pltpu.make_async_copy(src, dst, sem.at[i])
        for i, (src, dst) in enumerate(((rows, row_out), (cols, col_out)))
    ]
    for move in moves:
        move.start()
    for move in moves:
        move.wait()


def on_device(tiles, tile_brow, tile_bcol, tile_count):
    slots, width = tiles.shape[2], tiles.shape[3]
    brs = 32
    bcs = brs * (NZ * NC) // (NX * NY)
    piece = brs // NX
    f32 = jnp.float32
    vmem = pl.BlockSpec(memory_space=pltpu.VMEM)
    rows, cols = pl.pallas_call(
        kernel,
        out_shape=(
            jax.ShapeDtypeStruct((brs, 1, width), f32),
            jax.ShapeDtypeStruct((bcs, 1, width), f32),
        ),
        in_specs=[pl.BlockSpec(memory_space=pltpu.SMEM)] + [pl.BlockSpec(memory_space=pltpu.HBM)] * 3,
        out_specs=(vmem, vmem),
        scratch_shapes=[
            pltpu.SMEM((1, 1, slots), jnp.int32),
            pltpu.SMEM((1, 1, slots), jnp.int32),
            pltpu.VMEM((slots, width, width), jnp.bfloat16),
            pltpu.VMEM((slots, width, width), jnp.bfloat16),
            pltpu.VMEM((brs, width), f32),
            pltpu.VMEM((brs, width), f32),
            pltpu.VMEM((bcs, width), f32),
            pltpu.VMEM((bcs, width), f32),
            pltpu.VMEM((SWEEPS, brs, width), f32),
            pltpu.VMEM((SWEEPS, 2 * NX - 1, piece, width), f32),
            pltpu.VMEM((SWEEPS, PAIRS * NX, piece, width), f32),
            pltpu.VMEM((SWEEPS, NZ, bcs, width), f32),
            pltpu.VMEM((SWEEPS, bcs, width), f32),
            pltpu.VMEM((SWEEPS, bcs, width), f32),
            pltpu.SemaphoreType.REGULAR((2,)),
            pltpu.SemaphoreType.DMA((2,)),
            pltpu.SemaphoreType.DMA((slots // CHUNK,)),
            pltpu.SemaphoreType.DMA,
            pltpu.SemaphoreType.DMA((SWEEPS,)),
            pltpu.SemaphoreType.DMA((SWEEPS,)),
            pltpu.SemaphoreType.DMA((SWEEPS,)),
            pltpu.SemaphoreType.DMA((SWEEPS,)),
        ],
        name="equilibrate",
        compiler_params=pltpu.CompilerParams(
            collective_id=0, has_side_effects=True, vmem_limit_bytes=VMEM_LIMIT
        ),
    )(
        tile_count.reshape(1),
        *(
            pltpu.with_memory_space_constraint(a, pltpu.HBM)
            for a in (tile_brow, tile_bcol, tiles)
        ),
    )
    anywhere = pl.BlockSpec(memory_space=pltpu.HBM)
    return pl.pallas_call(
        finish,
        out_shape=(
            jax.ShapeDtypeStruct(rows.shape, f32),
            jax.ShapeDtypeStruct(cols.shape, f32),
        ),
        in_specs=[vmem, vmem],
        out_specs=(anywhere, anywhere),
        scratch_shapes=[pltpu.SemaphoreType.DMA((2,))],
        name="finish",
    )(*(pltpu.with_memory_space_constraint(a, pltpu.VMEM) for a in (rows, cols)))


def solution(mesh):
    in_specs = (
        P("prow", "pcol", None, None, None),
        P("prow", "pcol", None),
        P("prow", "pcol", None),
        P("prow", "pcol"),
    )
    out_specs = (P(None, "prow", None), P(None, "pcol", None))
    return jax.shard_map(
        on_device, mesh=mesh, in_specs=in_specs, out_specs=out_specs, check_vma=False
    )
```
